32 devices in a mesh: gx: 4 (over z), gy: 4 (over y, x), gz: 2 (over core).
Axes of the slice: x: 2, y: 2, z: 4, core: 2. Of those that a mesh axis runs over, the one named last changes fastest.
Arguments:
- chi_field: float32 [32, 128, 256], P('gx', 'gy', 'gz'), may hold values from 0.5 to 2.5, as said below
- metric: float32 [6, 32, 128, 256], P(None, 'gx', 'gy', 'gz'), may hold values from -0.3 to 1.5, as said below
- curvature: float32 [6, 32, 128, 256], P(None, 'gx', 'gy', 'gz'), may hold values from -1.6 to 1.6
- trace_curvature: float32 [32, 128, 256], P('gx', 'gy', 'gz'), may hold values from -3 to 3
- gamma_field: float32 [3, 32, 128, 256], P(None, 'gx', 'gy', 'gz'), may hold values from -1.6 to 1.6
Outputs:
- hamiltonian: float32 [32, 128, 256], P('gx', 'gy', 'gz')
- momentum: float32 [3, 32, 128, 256], P(None, 'gx', 'gy', 'gz')
- constraint_norms: float32 [2], replicated
The draws below stay inside these ranges and needn't reach their ends.
Inputs may be any that keep to these rules, and one draw needn't show every extreme that they name: `chi_field`: positive. `metric`: at every cell the symmetric 3x3 matrix built from the six components is positive definite with a dominant diagonal.
All inputs are finite; a program needn't handle non-finite values.
Results may differ from the reference program's by a relative error of at most 0.0003.
Values sent between devices are 32-bit elements; how exact they have to be, the bound alone decides.
No kernel may reach another device: no remote copies, remote signals or barrier semaphores. Data moves between devices by JAX's collectives and lax.ppermute only.
A program may use at most 128 MiB of HBM per device.

```python
import math
import jax
import jax.numpy as jnp
from jax import lax

CX = 8
NX = 32
NY = 128
NZ = 256
N_GX = 4


def ramp_level():
    xs = jnp.arange(NX, dtype=jnp.float32) / NX
    ys = jnp.arange(NY, dtype=jnp.float32) / NY
    zs = jnp.arange(NZ, dtype=jnp.float32) / NZ
    level = (xs[:, None, None] + ys[None, :, None] + zs[None, None, :]) / 3.0
    return jnp.exp(math.log(3.0) * level)


def draw_chi_field(key, part):
    noise = jax.random.uniform(key, (NX, NY, NZ), jnp.float32, -1.0, 1.0)
    value = 0.12 * ramp_level() * noise
    return jnp.exp(value)


def draw_metric(key, part):
    noise = jax.random.uniform(key, (6, NX, NY, NZ), jnp.float32, -1.0, 1.0)
    identity = jnp.array([1.0, 0.0, 0.0, 1.0, 0.0, 1.0], dtype=jnp.float32)[:, None, None, None]
    value = 0.05 * ramp_level()[None] * noise
    return identity + value


def draw_curvature(key, part):
    noise = jax.random.uniform(key, (6, NX, NY, NZ), jnp.float32, -1.0, 1.0)
    return 0.3 * ramp_level()[None] * noise


def draw_trace_curvature(key, part):
    noise = jax.random.uniform(key, (NX, NY, NZ), jnp.float32, -1.0, 1.0)
    value = 0.5 * ramp_level() * noise
    return value


def draw_gamma_field(key, part):
    noise = jax.random.uniform(key, (3, NX, NY, NZ), jnp.float32, -1.0, 1.0)
    return 0.3 * ramp_level()[None] * noise


def setup_inputs(seed: int = 0) -> dict:
    keys = jax.random.split(jax.random.key(seed), 6)
    return {
        "chi_field": draw_chi_field(jax.random.fold_in(keys[5], 71), 0),
        "metric": draw_metric(jax.random.fold_in(keys[5], 71), 0),
        "curvature": draw_curvature(jax.random.fold_in(keys[5], 71), 0),
        "trace_curvature": draw_trace_curvature(jax.random.fold_in(keys[5], 71), 0),
        "gamma_field": draw_gamma_field(jax.random.fold_in(keys[5], 71), 0),
    }


pair_index = ((0, 1, 2), (1, 3, 4), (2, 4, 5))
first_taps = ((-2, 1.0 / 12.0), (-1, -8.0 / 12.0), (1, 8.0 / 12.0), (2, -1.0 / 12.0))
second_taps = ((-2, -1.0 / 12.0), (-1, 16.0 / 12.0), (0, -30.0 / 12.0), (1, 16.0 / 12.0), (2, -1.0 / 12.0))

def window(padded, offsets):
    sx = padded.shape[-3] - 4
    sy = padded.shape[-2] - 4
    sz = padded.shape[-1] - 4
    return padded[..., 2 + offsets[0]:2 + offsets[0] + sx, 2 + offsets[1]:2 + offsets[1] + sy, 2 + offsets[2]:2 + offsets[2] + sz]

def shifted(pairs):
    places = [0, 0, 0]
    for axis_num, step in pairs:
        places[axis_num] = places[axis_num] + step
    return tuple(places)

def first_diff(padded, axis_num):
    summed = None
    for step, weight in first_taps:
        term = weight * window(padded, shifted(((axis_num, step),)))
        summed = term if summed is None else summed + term
    return summed

def second_diff(padded, a, b):
    summed = None
    if a == b:
        for step, weight in second_taps:
            term = weight * window(padded, shifted(((a, step),)))
            summed = term if summed is None else summed + term
        return summed
    for step_a, weight_a in first_taps:
        for step_b, weight_b in first_taps:
            term = weight_a * weight_b * window(padded, shifted(((a, step_a), (b, step_b))))
            summed = term if summed is None else summed + term
    return summed

def constraints(geo_pad, rest_pad):
    centre = window(geo_pad, (0, 0, 0))
    remainder = window(rest_pad, (0, 0, 0))
    conformal = centre[0]
    trace_curv = remainder[6]
    geo_first = [first_diff(geo_pad, a) for a in range(3)]
    rest_first = [first_diff(rest_pad, a) for a in range(3)]
    geo_second = {}
    for a in range(3):
        for b in range(a, 3):
            geo_second[a, b] = second_diff(geo_pad, a, b)

    def metric_at(i, j):
        return centre[1 + pair_index[i][j]]

    def curv_at(i, j):
        return remainder[pair_index[i][j]]

    def metric_grad(i, j, a):
        return geo_first[a][1 + pair_index[i][j]]

    def metric_hess(i, j, a, b):
        return geo_second[min(a, b), max(a, b)][1 + pair_index[i][j]]

    def chi_hess(a, b):
        return geo_second[min(a, b), max(a, b)][0]

    def curv_grad(i, j, a):
        return rest_first[a][pair_index[i][j]]
    chi_grad = [geo_first[a][0] for a in range(3)]
    trace_grad = [rest_first[a][6] for a in range(3)]
    g00, g01, g02 = (metric_at(0, 0), metric_at(0, 1), metric_at(0, 2))
    g11, g12, g22 = (metric_at(1, 1), metric_at(1, 2), metric_at(2, 2))
    minor00 = g11 * g22 - g12 * g12
    minor01 = g02 * g12 - g01 * g22
    minor02 = g01 * g12 - g02 * g11
    minor11 = g00 * g22 - g02 * g02
    minor12 = g01 * g02 - g00 * g12
    minor22 = g00 * g11 - g01 * g01
    determinant = g00 * minor00 + g01 * minor01 + g02 * minor02
    scale = 1.0 / determinant
    inverse_list = [minor00 * scale, minor01 * scale, minor02 * scale, minor11 * scale, minor12 * scale, minor22 * scale]

    def inv_at(i, j):
        return inverse_list[pair_index[i][j]]
    christ_low = [[[None] * 3 for i in range(3)] for k in range(3)]
    for k in range(3):
        for i in range(3):
            for j in range(i, 3):
                value = 0.5 * (metric_grad(k, j, i) + metric_grad(k, i, j) - metric_grad(i, j, k))
                christ_low[k][i][j] = value
                christ_low[k][j][i] = value
    christ_up = [[[None] * 3 for i in range(3)] for k in range(3)]
    for k in range(3):
        for i in range(3):
            for j in range(i, 3):
                value = inv_at(k, 0) * christ_low[0][i][j] + inv_at(k, 1) * christ_low[1][i][j] + inv_at(k, 2) * christ_low[2][i][j]
                christ_up[k][i][j] = value
                christ_up[k][j][i] = value
    gamma_calc = []
    for k in range(3):
        summed = None
        for i in range(3):
            for j in range(3):
                term = inv_at(i, j) * christ_up[k][i][j]
                summed = term if summed is None else summed + term
        gamma_calc.append(summed)
    cov_hess = [[None] * 3 for i in range(3)]
    for i in range(3):
        for j in range(i, 3):
            value = chi_hess(i, j) - (christ_up[0][i][j] * chi_grad[0] + christ_up[1][i][j] * chi_grad[1] + christ_up[2][i][j] * chi_grad[2])
            cov_hess[i][j] = value
            cov_hess[j][i] = value
    laplace = None
    grad_sq = None
    for l in range(3):
        for m in range(3):
            term = inv_at(l, m) * cov_hess[l][m]
            laplace = term if laplace is None else laplace + term
            term = inv_at(l, m) * chi_grad[l] * chi_grad[m]
            grad_sq = term if grad_sq is None else grad_sq + term
    scalar_sum = None
    for i in range(3):
        for j in range(i, 3):
            ricci = None
            for l in range(3):
                for m in range(3):
                    term = -0.5 * inv_at(l, m) * metric_hess(i, j, l, m)
                    ricci = term if ricci is None else ricci + term
            for k in range(3):
                ricci = ricci + 0.5 * (metric_at(k, i) * rest_first[j][7 + k] + metric_at(k, j) * rest_first[i][7 + k])
                ricci = ricci + 0.5 * gamma_calc[k] * (christ_low[i][j][k] + christ_low[j][i][k])
            for l in range(3):
                for m in range(3):
                    inner = None
                    for k in range(3):
                        term = christ_up[k][l][i] * christ_low[j][k][m] + christ_up[k][l][j] * christ_low[i][k][m] + christ_up[k][i][m] * christ_low[k][l][j]
                        inner = term if inner is None else inner + term
                    ricci = ricci + inv_at(l, m) * inner
            conf_part = (cov_hess[i][j] + metric_at(i, j) * laplace) / (2.0 * conformal) - (chi_grad[i] * chi_grad[j] + 3.0 * metric_at(i, j) * grad_sq) / (4.0 * conformal * conformal)
            weight = 1.0 if i == j else 2.0
            term = weight * inv_at(i, j) * (ricci + conf_part)
            scalar_sum = term if scalar_sum is None else scalar_sum + term
    mixed = [[None] * 3 for i in range(3)]
    for i in range(3):
        for j in range(3):
            mixed[i][j] = curv_at(i, 0) * inv_at(0, j) + curv_at(i, 1) * inv_at(1, j) + curv_at(i, 2) * inv_at(2, j)
    square_sum = None
    for i in range(3):
        for j in range(3):
            term = mixed[i][j] * mixed[j][i]
            square_sum = term if square_sum is None else square_sum + term
    hamilton = conformal * scalar_sum + 2.0 / 3.0 * trace_curv * trace_curv - square_sum
    momentum_list = []
    for i in range(3):
        summed = None
        for j in range(3):
            for k in range(3):
                term = inv_at(j, k) * curv_grad(k, i, j)
                summed = term if summed is None else summed + term
        for l in range(3):
            summed = summed - gamma_calc[l] * curv_at(l, i)
            for j in range(3):
                summed = summed - christ_up[l][j][i] * mixed[l][j]
        along = mixed[i][0] * chi_grad[0] + mixed[i][1] * chi_grad[1] + mixed[i][2] * chi_grad[2]
        summed = summed - 2.0 / 3.0 * trace_grad[i] - 1.5 * along / conformal
        momentum_list.append(summed)
    return (hamilton, jnp.stack(momentum_list))

def reference(chi_field, metric, curvature, trace_curvature, gamma_field):
    geometry = jnp.concatenate([chi_field[None], metric], 0)
    remainder = jnp.concatenate([curvature, trace_curvature[None], gamma_field], 0)
    geo_pad = jnp.pad(geometry, ((0, 0), (2, 2), (2, 2), (2, 2)), mode='wrap')
    rest_pad = jnp.pad(remainder, ((0, 0), (2, 2), (2, 2), (2, 2)), mode='wrap')

    def one_slab(index):
        start = (index * CX).astype(jnp.int32)
        geo_slab = lax.dynamic_slice_in_dim(geo_pad, start, CX + 4, 1)
        rest_slab = lax.dynamic_slice_in_dim(rest_pad, start, CX + 4, 1)
        hamilton, momentum = constraints(geo_slab, rest_slab)
        ham_sq = lax.optimization_barrier(jnp.sum(lax.optimization_barrier(jnp.sum(lax.optimization_barrier(jnp.sum(hamilton * hamilton, axis=2)), axis=1)), axis=0))
        mom_sq = lax.optimization_barrier(jnp.sum(lax.optimization_barrier(jnp.sum(lax.optimization_barrier(jnp.sum(lax.optimization_barrier(jnp.sum(momentum * momentum, axis=3)), axis=2)), axis=1)), axis=0))
        return (hamilton, momentum, ham_sq, mom_sq)
    hamilton, momentum, ham_sq, mom_sq = lax.map(one_slab, jnp.arange(N_GX, dtype=jnp.int32))
    hamilton = hamilton.reshape(chi_field.shape)
    momentum = jnp.moveaxis(momentum, 1, 0).reshape(gamma_field.shape)
    cell_count = chi_field.size
    sums = jnp.stack([jnp.sum(ham_sq), jnp.sum(mom_sq)])
    norms = jnp.sqrt(sums / jnp.array([cell_count, 3 * cell_count], dtype=jnp.float32))
    return (hamilton, momentum, norms)
```

```python
import functools

import jax
import jax.numpy as jnp
from jax import lax
from jax.experimental import pallas as pl
from jax.experimental.pallas import tpu as pltpu
from jax.sharding import PartitionSpec as P

AXES = ("gx", "gy", "gz")
PAIR = ((0, 1, 2), (1, 3, 4), (2, 4, 5))
GEO = 7


def pack_kernel(chi, met, cur, tra, gam, out):
    planes, rows, lanes = chi.shape
    tiles = rows // 8
    lane = lax.broadcasted_iota(jnp.int32, (8, lanes), 1)

    def pack(ref, lead):
        acc = jnp.zeros((8, lanes), jnp.float32)
        for p in range(planes):
            for t in range(tiles):
                k = 4 * (p * tiles + t)
                tile = ref[lead + (p, slice(8 * t, 8 * t + 8))]
                moved = pltpu.roll(tile, k + 2, 1) if k + 2 < lanes else tile
                acc = jnp.where((lane >= k) & (lane < k + 4), moved, acc)
        return acc

    out[0] = pack(chi, ())

    def six(c, _):
        out[1 + c] = pack(met, (c,))
        out[7 + c] = pack(cur, (c,))
        return 0

    lax.fori_loop(0, 6, six, 0)
    out[13] = pack(tra, ())
    out[14] = pack(gam, (2,))


def pieces_of(start, count, planes):
    cuts = sorted({start - 2, 0, start, start + count, planes, start + count + 2})
    cuts = [c for c in cuts if start - 2 <= c <= start + count + 2]
    return [
        (a, b, "lo" if b <= 0 else ("hi" if a >= planes else "mid"), a >= start and b <= start + count)
        for a, b in zip(cuts[:-1], cuts[1:])
    ]


def main_kernel(
    groups, planes, rows, lanes, devices,
    chi, met, cur, tra, gam, xlo_g, xhi_g, xlo_r, xhi_r,
    ylo, yhi, yxlo, yxhi, pz, pylo, pyhi, pxlo, pxhi,
    ham_out, mom_out, sums_out,
    F, GZ, DZ, DY, QZ, O, sems, osem,
):
    tiles = rows // 8
    lane = lax.broadcasted_iota(jnp.int32, (8, lanes), 1)
    copies = []

    def fetch(src, dst):
        copies.append(pltpu.make_async_copy(src, dst, sems.at[len(copies)]))

    mid = pl.ds(8, rows)
    base = 0
    obase = 0
    plan = []
    for start, count in groups:
        for a, b, kind, is_out in pieces_of(start, count, planes):
            at = pl.ds(base + a - start + 2, b - a)
            plan.append((base + a - start + 2, a, b - a, kind, is_out, obase + a - start))
            if kind == "mid":
                s = pl.ds(a, b - a)
                fetch(chi.at[s], F.at[0, at, mid])
                fetch(met.at[:, s], F.at[pl.ds(1, 6), at, mid])
                fetch(cur.at[:, s], F.at[pl.ds(7, 6), at, mid])
                fetch(tra.at[s], F.at[13, at, mid])
                fetch(gam.at[pl.ds(0, 2), s], F.at[pl.ds(14, 2), at, mid])
                if is_out:
                    fetch(gam.at[2, s], GZ.at[pl.ds(obase + a - start, b - a)])
            else:
                geo, rest = (xlo_g, xlo_r) if kind == "lo" else (xhi_g, xhi_r)
                fetch(geo, F.at[pl.ds(0, 7), at, mid])
                fetch(rest, F.at[pl.ds(7, 8), at, mid])
        base += count + 4
        obase += count
    for c in copies:
        c.start()
    for bp, s, n, kind, is_out, ob in plan:
        at = slice(bp, bp + n)
        if kind == "mid":
            ss = slice(s, s + n)
            F[0:14, at, 6:8, :] = ylo[0:14, ss]
            F[0:14, at, 8 + rows : 10 + rows, :] = yhi[0:14, ss]
            F[15, at, 6:8, :] = ylo[14, ss]
            F[15, at, 8 + rows : 10 + rows, :] = yhi[14, ss]
        else:
            src = yxlo if kind == "lo" else yxhi
            F[0:7, at, 6:8, :] = src[0]
            F[0:7, at, 8 + rows : 10 + rows, :] = src[1]
    for c in copies:
        c.wait()

    def neighbours(x, h):
        p1 = pltpu.roll(jnp.where(lane < 1, h, x), lanes - 1, 1)
        p2 = pltpu.roll(jnp.where(lane < 2, h, x), lanes - 2, 1)
        m1 = pltpu.roll(jnp.where(lane >= lanes - 1, h, x), 1, 1)
        m2 = pltpu.roll(jnp.where(lane >= lanes - 2, h, x), 2, 1)
        return p1, p2, m1, m2

    def edge(tile, k):
        return pltpu.roll(tile, lanes - 2 - 4 * k, 1)

    def slope(p1, p2, m1, m2):
        return (p1 - m1) - 0.125 * (p2 - m2)

    def bend(x, p1, p2, m1, m2):
        return (p1 + m1) - 0.0625 * (p2 + m2) - 1.875 * x

    for bp0, s0, n, kind, is_out, ob0 in plan:
        psrc = {"lo": pxlo, "hi": pxhi, "mid": pz}[kind]
        soff = {"lo": planes, "hi": -planes, "mid": 0}[kind]

        def first_pass(i, _, bp0=bp0, s0=s0, is_out=is_out, ob0=ob0, psrc=psrc, soff=soff):
            bp = bp0 + i
            s = s0 + soff + i
            for f in range(GEO):
                for t in range(tiles):
                    r = 8 + 8 * t
                    x = F[f, bp, r : r + 8, :]
                    nb = neighbours(x, edge(psrc[f], s * tiles + t))
                    DZ[f, bp, r : r + 8, :] = slope(*nb)
                    if is_out:
                        QZ[f, ob0 + i, 8 * t : 8 * t + 8, :] = bend(x, *nb)
                    DY[f, bp, 8 * t : 8 * t + 8, :] = slope(
                        *(F[f, bp, r + d : r + d + 8, :] for d in (1, 2, -1, -2))
                    )
                if is_out:
                    for r, src, t in ((0, pylo, tiles - 1), (8 + rows, pyhi, 0)):
                        x = F[f, bp, r : r + 8, :]
                        nb = neighbours(x, edge(src[f], s * tiles + t))
                        DZ[f, bp, r : r + 8, :] = slope(*nb)
            return 0

        lax.fori_loop(0, n, first_pass, 0)

    def cell(bp, sp, op, t):
        r = 8 + 8 * t
        k = sp * tiles + t

        def at(f, dx=0, dy=0):
            return F[f, bp + dx, r + dy : r + dy + 8, :]

        g = [at(1 + c) for c in range(6)]
        m00 = g[3] * g[5] - g[4] * g[4]
        m01 = g[2] * g[4] - g[1] * g[5]
        m02 = g[1] * g[4] - g[2] * g[3]
        m11 = g[0] * g[5] - g[2] * g[2]
        m12 = g[1] * g[2] - g[0] * g[4]
        m22 = g[0] * g[3] - g[1] * g[1]
        scale = 1.0 / (g[0] * m00 + g[1] * m01 + g[2] * m02)
        u = [m * scale for m in (m00, m01, m02, m11, m12, m22)]
        U = [[u[PAIR[i][j]] for j in range(3)] for i in range(3)]
        half = [(2.0 / 3.0) * u[c] for c in (1, 2, 4)]

        def dot_sym(w, v):
            return (w[0] * v[0] + w[3] * v[3] + w[5] * v[5]) + 2.0 * (
                w[1] * v[1] + w[2] * v[2] + w[4] * v[4]
            )

        def geometry(f):
            x = at(f)
            xs = [at(f, dx=d) for d in (1, 2, -1, -2)]
            ys = [at(f, dy=d) for d in (1, 2, -1, -2)]
            ex = slope(*xs)
            ey = DY[f, bp, 8 * t : 8 * t + 8, :]
            ez = DZ[f, bp, r : r + 8, :]
            exy = slope(*(DY[f, bp + d, 8 * t : 8 * t + 8, :] for d in (1, 2, -1, -2)))
            exz = slope(*(DZ[f, bp + d, r : r + 8, :] for d in (1, 2, -1, -2)))
            eyz = slope(*(DZ[f, bp, r + d : r + d + 8, :] for d in (1, 2, -1, -2)))
            box = u[0] * bend(x, *xs) + u[3] * bend(x, *ys)
            box = box + u[5] * QZ[f, op, 8 * t : 8 * t + 8, :]
            box = box + (half[0] * exy + half[1] * exz + half[2] * eyz)
            return (ex, ey, ez), box

        E = [None] * 6
        boxes = [None] * 6
        for c in range(6):
            E[c], boxes[c] = geometry(1 + c)
        box_metric = dot_sym(u, boxes)
        ec, box_chi = geometry(0)
        dchi = [(2.0 / 3.0) * e for e in ec]

        L = [[None] * 6 for _ in range(3)]
        for kk in range(3):
            for i in range(3):
                for j in range(i, 3):
                    L[kk][PAIR[i][j]] = (E[PAIR[kk][j]][i] + E[PAIR[kk][i]][j]) - E[PAIR[i][j]][kk]
        us = [(1.0 / 3.0) * v for v in u]
        US = [[us[PAIR[i][j]] for j in range(3)] for i in range(3)]
        C = [
            [US[kk][0] * L[0][c] + US[kk][1] * L[1][c] + US[kk][2] * L[2][c] for c in range(6)]
            for kk in range(3)
        ]
        gd = [dot_sym(u, C[kk]) for kk in range(3)]
        trace_grad = [dot_sym(us, [E[c][kk] for c in range(6)]) for kk in range(3)]

        def pair_trace(A, B, same):
            if same:
                return (A[0][0] * A[0][0] + A[1][1] * A[1][1] + A[2][2] * A[2][2]) + 2.0 * (
                    A[0][1] * A[1][0] + A[0][2] * A[2][0] + A[1][2] * A[2][1]
                )
            total = None
            for a in range(3):
                for b in range(3):
                    term = A[a][b] * B[b][a]
                    total = term if total is None else total + term
            return total

        def contract(mats):
            return dot_sym(
                u,
                [
                    pair_trace(mats[i], mats[j], i == j)
                    for i, j in ((0, 0), (0, 1), (0, 2), (1, 1), (1, 2), (2, 2))
                ],
            )

        quad_c = contract([[[C[kk][PAIR[l][i]] for i in range(3)] for kk in range(3)] for l in range(3)])
        Z = [
            [
                [
                    US[i][0] * L[n][PAIR[0][j]] + US[i][1] * L[n][PAIR[1][j]] + US[i][2] * L[n][PAIR[2][j]]
                    for j in range(3)
                ]
                for i in range(3)
            ]
            for n in range(3)
        ]
        quad_z = contract(Z)
        div = slope(*(at(14, dx=d) for d in (1, 2, -1, -2))) + slope(
            *(at(15, dy=d) for d in (1, 2, -1, -2))
        )
        div = div + slope(
            *neighbours(GZ[op, 8 * t : 8 * t + 8, :], edge(pz[14], k))
        )
        ricci = (2.0 / 3.0) * (div - box_metric)
        ricci = ricci + (gd[0] * trace_grad[0] + gd[1] * trace_grad[1] + gd[2] * trace_grad[2])
        ricci = ricci + 2.0 * quad_c + quad_z

        chi_c = at(0)
        inv_chi = 1.0 / chi_c
        laplace = (4.0 / 3.0) * box_chi - (gd[0] * dchi[0] + gd[1] * dchi[1] + gd[2] * dchi[2])
        grad_sq = (
            u[0] * dchi[0] * dchi[0] + u[3] * dchi[1] * dchi[1] + u[5] * dchi[2] * dchi[2]
        ) + 2.0 * (
            u[1] * dchi[0] * dchi[1] + u[2] * dchi[0] * dchi[2] + u[4] * dchi[1] * dchi[2]
        )
        A = [at(7 + c) for c in range(6)]
        mixed = [
            [
                A[PAIR[i][0]] * U[0][j] + A[PAIR[i][1]] * U[1][j] + A[PAIR[i][2]] * U[2][j]
                for j in range(3)
            ]
            for i in range(3)
        ]
        K = at(13)
        ham = chi_c * ricci + 2.0 * laplace - 2.5 * grad_sq * inv_chi
        ham = ham + (2.0 / 3.0) * K * K - pair_trace(mixed, mixed, True)
        O[0, op, 8 * t : 8 * t + 8, :] = ham

        EA = []
        for c in range(7):
            f = 7 + c
            EA.append(
                (
                    slope(*(at(f, dx=d) for d in (1, 2, -1, -2))),
                    slope(*(at(f, dy=d) for d in (1, 2, -1, -2))),
                    slope(*neighbours(at(f), edge(pz[f], k))),
                )
            )
        weighted = [1.5 * inv_chi * d for d in dchi]
        mom_sq = None
        for i in range(3):
            flat = None
            for j in range(3):
                for m in range(3):
                    term = U[j][m] * EA[PAIR[m][i]][j]
                    flat = term if flat is None else flat + term
            total = (2.0 / 3.0) * (flat - (2.0 / 3.0) * EA[6][i])
            for l in range(3):
                total = total - gd[l] * A[PAIR[l][i]]
                for j in range(3):
                    total = total - C[l][PAIR[j][i]] * mixed[l][j]
                total = total - mixed[i][l] * weighted[l]
            O[1 + i, op, 8 * t : 8 * t + 8, :] = total
            mom_sq = total * total if mom_sq is None else mom_sq + total * total
        return ham * ham, mom_sq

    zero = jnp.zeros((8, lanes), jnp.float32)
    acc = (zero, zero)
    writes = []
    base = 0
    obase = 0
    for start, count in groups:

        def one_plane(i, acc, base=base, obase=obase, start=start):
            for t in range(tiles):
                h, m = cell(base + 2 + i, start + i, obase + i, t)
                acc = (acc[0] + h, acc[1] + m)
            return acc

        acc = lax.fori_loop(0, count, one_plane, acc)
        src = pl.ds(obase, count)
        dst = pl.ds(start, count)
        writes.append(pltpu.make_async_copy(O.at[0, src], ham_out.at[dst], osem.at[len(writes)]))
        writes[-1].start()
        writes.append(
            pltpu.make_async_copy(O.at[pl.ds(1, 3), src], mom_out.at[:, dst], osem.at[len(writes)])
        )
        writes[-1].start()
        base += count + 4
        obase += count
    h = jnp.sum(acc[0], axis=0, keepdims=True)
    m = jnp.sum(acc[1], axis=0, keepdims=True)
    half_lane = lanes // 2
    row = lax.broadcasted_iota(jnp.int32, (1, lanes), 1)
    row = jnp.where(row < half_lane, h + pltpu.roll(h, half_lane, 1), m + pltpu.roll(m, half_lane, 1))
    sums_out[...] = jnp.broadcast_to(row, (devices, lanes))
    for w in writes:
        w.wait()


def hop(value, axis, step):
    n = lax.axis_size(axis)
    return lax.ppermute(value, axis, [(i, (i + step) % n) for i in range(n)])


def on_device(chi, met, cur, tra, gam):
    planes, rows, lanes = chi.shape
    devices = lax.axis_size(AXES)
    f32 = jnp.float32
    any_spec = pl.BlockSpec(memory_space=pl.ANY)
    vmem = pl.BlockSpec(memory_space=pltpu.VMEM)

    def x_geo(s):
        return jnp.concatenate([chi[None, s], met[:, s]], 0)

    def x_rest(s):
        return jnp.concatenate([cur[:, s], tra[None, s], gam[:1, s]], 0)

    def y_all(s):
        return jnp.concatenate([chi[None, :, s], met[:, :, s], cur[:, :, s], tra[None, :, s], gam[1:2, :, s]], 0)

    first, last = slice(0, 2), slice(planes - 2, planes)
    yfirst, ylast = slice(0, 2), slice(rows - 2, rows)
    xlo_g = hop(x_geo(last), "gx", 1)
    xhi_g = hop(x_geo(first), "gx", -1)
    packed = pl.pallas_call(
        pack_kernel,
        out_shape=jax.ShapeDtypeStruct((15, 8, lanes), f32),
        in_specs=[vmem] * 5,
        out_specs=vmem,
        name="pack_z",
    )(chi, met, cur, tra, gam)
    if lax.axis_size("gz") == 2:
        pz = hop(packed, "gz", 1)
    else:
        up = hop(packed, "gz", 1)
        down = hop(packed, "gz", -1)
        pz = jnp.where(lax.broadcasted_iota(jnp.int32, packed.shape, 2) % 4 < 2, up, down)
    ylo = hop(y_all(ylast), "gy", 1)
    yhi = hop(y_all(yfirst), "gy", -1)
    xlo_r = hop(x_rest(last), "gx", 1)
    xhi_r = hop(x_rest(first), "gx", -1)
    geo_z = pz[:GEO]
    pylo = hop(geo_z, "gy", 1)
    pyhi = hop(geo_z, "gy", -1)
    pxlo = hop(geo_z, "gx", 1)
    pxhi = hop(geo_z, "gx", -1)
    yxlo = hop(jnp.stack([ylo[:GEO, last], yhi[:GEO, last]]), "gx", 1)
    yxhi = hop(jnp.stack([ylo[:GEO, first], yhi[:GEO, first]]), "gx", -1)

    groups = ((0, planes),)
    buf = sum(c + 4 for _, c in groups)
    outs = sum(c for _, c in groups)
    pad_rows = rows + 16
    ham, mom, sums = pl.pallas_call(
        functools.partial(main_kernel, groups, planes, rows, lanes, devices),
        out_shape=(
            jax.ShapeDtypeStruct(chi.shape, f32),
            jax.ShapeDtypeStruct(gam.shape, f32),
            jax.ShapeDtypeStruct((devices, lanes), f32),
        ),
        in_specs=[any_spec] * 9 + [vmem] * 9,
        out_specs=(any_spec, any_spec, vmem),
        scratch_shapes=[
            pltpu.VMEM((16, buf, pad_rows, lanes), f32),
            pltpu.VMEM((outs, rows, lanes), f32),
            pltpu.VMEM((GEO, buf, pad_rows, lanes), f32),
            pltpu.VMEM((GEO, buf, rows, lanes), f32),
            pltpu.VMEM((GEO, outs, rows, lanes), f32),
            pltpu.VMEM((4, outs, rows, lanes), f32),
            pltpu.SemaphoreType.DMA((32,)),
            pltpu.SemaphoreType.DMA((2 * len(groups),)),
        ],
        name="constraints",
    )(chi, met, cur, tra, gam, xlo_g, xhi_g, xlo_r, xhi_r, ylo, yhi, yxlo, yxhi, pz, pylo, pyhi, pxlo, pxhi)
    parts = jnp.sum(lax.all_to_all(sums, AXES, 0, 0, tiled=True), axis=0)
    totals = jnp.stack([jnp.sum(parts[: lanes // 2]), jnp.sum(parts[lanes // 2 :])])
    cells = chi.size * devices
    norms = jnp.sqrt(totals / jnp.array([cells, 3 * cells], dtype=f32))
    return ham, mom, norms


def solution(mesh):
    return jax.shard_map(
        on_device,
        mesh=mesh,
        in_specs=(
            P("gx", "gy", "gz"),
            P(None, "gx", "gy", "gz"),
            P(None, "gx", "gy", "gz"),
            P("gx", "gy", "gz"),
            P(None, "gx", "gy", "gz"),
        ),
        out_specs=(P("gx", "gy", "gz"), P(None, "gx", "gy", "gz"), P()),
        check_vma=False,
    )
```

```python
import functools

import jax
import jax.numpy as jnp
from jax import lax
from jax.experimental import pallas as pl
from jax.experimental.pallas import tpu as pltpu
from jax.sharding import PartitionSpec as P

AXES = ("gx", "gy", "gz")
PAIR = ((0, 1, 2), (1, 3, 4), (2, 4, 5))
GEO = 7


def pack_kernel(chi, met, cur, tra, gam, out):
    planes, rows, lanes = chi.shape
    tiles = rows // 8
    lane = lax.broadcasted_iota(jnp.int32, (8, lanes), 1)

    def pack(ref, lead):
        acc = jnp.zeros((8, lanes), jnp.float32)
        for p in range(planes):
            for t in range(tiles):
                k = 4 * (p * tiles + t)
                tile = ref[lead + (p, slice(8 * t, 8 * t + 8))]
                moved = pltpu.roll(tile, k + 2, 1) if k + 2 < lanes else tile
                acc = jnp.where((lane >= k) & (lane < k + 4), moved, acc)
        return acc

    out[0] = pack(chi, ())

    def six(c, _):
        out[1 + c] = pack(met, (c,))
        out[7 + c] = pack(cur, (c,))
        return 0

    lax.fori_loop(0, 6, six, 0)
    out[13] = pack(tra, ())
    out[14] = pack(gam, (2,))


def pieces_of(start, count, planes):
    cuts = sorted({start - 2, 0, start, start + count, planes, start + count + 2})
    cuts = [c for c in cuts if start - 2 <= c <= start + count + 2]
    return [
        (a, b, "lo" if b <= 0 else ("hi" if a >= planes else "mid"), a >= start and b <= start + count)
        for a, b in zip(cuts[:-1], cuts[1:])
    ]


def main_kernel(
    groups, edges, planes, rows, lanes, devices,
    *refs,
):
    chi, met, cur, tra, gam, ylo, yhi, pz, pylo, pyhi = refs[:10]
    refs = refs[10:]
    if edges:
        xlo, xhi, sxlo, sxhi, before = refs[:5]
        refs = refs[7:]
    ham_out, mom_out, sums_out, F, GZ, DZ, DY, QZ, O, sems, osem = refs
    tiles = rows // 8
    lane = lax.broadcasted_iota(jnp.int32, (8, lanes), 1)
    copies = []

    def fetch(src, dst):
        copies.append(pltpu.make_async_copy(src, dst, sems.at[len(copies)]))

    mid = pl.ds(8, rows)
    base = 0
    obase = 0
    plan = []
    for start, count in groups:
        for a, b, kind, is_out in pieces_of(start, count, planes):
            at = pl.ds(base + a - start + 2, b - a)
            plan.append((base + a - start + 2, a, b - a, kind, is_out, obase + a - start))
            if kind == "mid":
                s = pl.ds(a, b - a)
                fetch(chi.at[s], F.at[0, at, mid])
                fetch(met.at[:, s], F.at[pl.ds(1, 6), at, mid])
                fetch(cur.at[:, s], F.at[pl.ds(7, 6), at, mid])
                fetch(tra.at[s], F.at[13, at, mid])
                fetch(gam.at[pl.ds(0, 2), s], F.at[pl.ds(14, 2), at, mid])
                if is_out:
                    fetch(gam.at[2, s], GZ.at[pl.ds(obase + a - start, b - a)])
            else:
                fetch(xlo if kind == "lo" else xhi, F.at[pl.ds(0, 15), at, mid])
        base += count + 4
        obase += count
    for c in copies:
        c.start()
    for bp, s, n, kind, is_out, ob in plan:
        at = slice(bp, bp + n)
        if kind == "mid":
            ss = slice(s, s + n)
            F[0:14, at, 6:8, :] = ylo[0:14, ss]
            F[0:14, at, 8 + rows : 10 + rows, :] = yhi[0:14, ss]
            F[15, at, 6:8, :] = ylo[14, ss]
            F[15, at, 8 + rows : 10 + rows, :] = yhi[14, ss]
        else:
            src = sxlo if kind == "lo" else sxhi
            for i in range(n):
                F[0:7, bp + i, 6:8, :] = src[7:14, 2 * i : 2 * i + 2]
                F[0:7, bp + i, 8 + rows : 10 + rows, :] = src[7:14, 4 + 2 * i : 6 + 2 * i]
    for c in copies:
        c.wait()

    def neighbours(x, h):
        p1 = pltpu.roll(jnp.where(lane < 1, h, x), lanes - 1, 1)
        p2 = pltpu.roll(jnp.where(lane < 2, h, x), lanes - 2, 1)
        m1 = pltpu.roll(jnp.where(lane >= lanes - 1, h, x), 1, 1)
        m2 = pltpu.roll(jnp.where(lane >= lanes - 2, h, x), 2, 1)
        return p1, p2, m1, m2

    def edge(tile, k):
        return pltpu.roll(tile, lanes - 2 - 4 * k, 1)

    def slope(p1, p2, m1, m2):
        return (p1 - m1) - 0.125 * (p2 - m2)

    def bend(x, p1, p2, m1, m2):
        return (p1 + m1) - 0.0625 * (p2 + m2) - 1.875 * x

    for bp0, s0, n, kind, is_out, ob0 in plan:
        psrc = pz if kind == "mid" else (sxlo if kind == "lo" else sxhi)
        soff = {"lo": planes, "hi": -planes, "mid": 0}[kind]

        def first_pass(i, _, bp0=bp0, s0=s0, is_out=is_out, ob0=ob0, psrc=psrc, soff=soff):
            bp = bp0 + i
            s = s0 + soff + i
            spots = [(8 + 8 * t, psrc, t) for t in range(tiles)]
            if is_out:
                spots += [(0, pylo, tiles - 1), (8 + rows, pyhi, 0)]
            ends = [[edge(src[f], s * tiles + t) for _, src, t in spots] for f in range(GEO)]

            def moves(f):
                return [neighbours(F[f, bp, r : r + 8, :], h) for (r, _, _), h in zip(spots, ends[f])]

            moved = moves(0)
            for f in range(GEO):
                ahead = moves(f + 1) if f + 1 < GEO else None
                for t in range(tiles):
                    r = 8 + 8 * t
                    DY[f, bp, 8 * t : 8 * t + 8, :] = slope(
                        *(F[f, bp, r + d : r + d + 8, :] for d in (1, 2, -1, -2))
                    )
                for n_spot, (r, _, t) in enumerate(spots):
                    DZ[f, bp, r : r + 8, :] = slope(*moved[n_spot])
                    if is_out and n_spot < tiles:
                        QZ[f, ob0 + i, 8 * t : 8 * t + 8, :] = bend(F[f, bp, r : r + 8, :], *moved[n_spot])
                moved = ahead
            return 0

        lax.fori_loop(0, n, first_pass, 0)

    def cell(bp, sp, op, t):
        r = 8 + 8 * t
        k = sp * tiles + t

        def at(f, dx=0, dy=0):
            return F[f, bp + dx, r + dy : r + dy + 8, :]

        g = [at(1 + c) for c in range(6)]
        m00 = g[3] * g[5] - g[4] * g[4]
        m01 = g[2] * g[4] - g[1] * g[5]
        m02 = g[1] * g[4] - g[2] * g[3]
        m11 = g[0] * g[5] - g[2] * g[2]
        m12 = g[1] * g[2] - g[0] * g[4]
        m22 = g[0] * g[3] - g[1] * g[1]
        scale = 1.0 / (g[0] * m00 + g[1] * m01 + g[2] * m02)
        u = [m * scale for m in (m00, m01, m02, m11, m12, m22)]
        U = [[u[PAIR[i][j]] for j in range(3)] for i in range(3)]
        half = [(2.0 / 3.0) * u[c] for c in (1, 2, 4)]

        def dot_sym(w, v):
            return (w[0] * v[0] + w[3] * v[3] + w[5] * v[5]) + 2.0 * (
                w[1] * v[1] + w[2] * v[2] + w[4] * v[4]
            )

        def geometry(f):
            x = at(f)
            xs = [at(f, dx=d) for d in (1, 2, -1, -2)]
            ys = [at(f, dy=d) for d in (1, 2, -1, -2)]
            ex = slope(*xs)
            ey = DY[f, bp, 8 * t : 8 * t + 8, :]
            ez = DZ[f, bp, r : r + 8, :]
            exy = slope(*(DY[f, bp + d, 8 * t : 8 * t + 8, :] for d in (1, 2, -1, -2)))
            exz = slope(*(DZ[f, bp + d, r : r + 8, :] for d in (1, 2, -1, -2)))
            eyz = slope(*(DZ[f, bp, r + d : r + d + 8, :] for d in (1, 2, -1, -2)))
            box = u[0] * bend(x, *xs) + u[3] * bend(x, *ys)
            box = box + u[5] * QZ[f, op, 8 * t : 8 * t + 8, :]
            box = box + (half[0] * exy + half[1] * exz + half[2] * eyz)
            return (ex, ey, ez), box

        E = [None] * 6
        boxes = [None] * 6
        for c in range(6):
            E[c], boxes[c] = geometry(1 + c)
        box_metric = dot_sym(u, boxes)
        ec, box_chi = geometry(0)
        dchi = [(2.0 / 3.0) * e for e in ec]

        L = [[None] * 6 for _ in range(3)]
        for kk in range(3):
            for i in range(3):
                for j in range(i, 3):
                    L[kk][PAIR[i][j]] = (E[PAIR[kk][j]][i] + E[PAIR[kk][i]][j]) - E[PAIR[i][j]][kk]
        us = [(1.0 / 3.0) * v for v in u]
        US = [[us[PAIR[i][j]] for j in range(3)] for i in range(3)]
        C = [
            [US[kk][0] * L[0][c] + US[kk][1] * L[1][c] + US[kk][2] * L[2][c] for c in range(6)]
            for kk in range(3)
        ]
        gd = [dot_sym(u, C[kk]) for kk in range(3)]
        trace_grad = [dot_sym(us, [E[c][kk] for c in range(6)]) for kk in range(3)]

        def pair_trace(A, B, same):
            if same:
                return (A[0][0] * A[0][0] + A[1][1] * A[1][1] + A[2][2] * A[2][2]) + 2.0 * (
                    A[0][1] * A[1][0] + A[0][2] * A[2][0] + A[1][2] * A[2][1]
                )
            total = None
            for a in range(3):
                for b in range(3):
                    term = A[a][b] * B[b][a]
                    total = term if total is None else total + term
            return total

        def contract(mats):
            return dot_sym(
                u,
                [
                    pair_trace(mats[i], mats[j], i == j)
                    for i, j in ((0, 0), (0, 1), (0, 2), (1, 1), (1, 2), (2, 2))
                ],
            )

        quad_c = contract([[[C[kk][PAIR[l][i]] for i in range(3)] for kk in range(3)] for l in range(3)])
        Z = [
            [
                [
                    US[i][0] * L[n][PAIR[0][j]] + US[i][1] * L[n][PAIR[1][j]] + US[i][2] * L[n][PAIR[2][j]]
                    for j in range(3)
                ]
                for i in range(3)
            ]
            for n in range(3)
        ]
        quad_z = contract(Z)
        div = slope(*(at(14, dx=d) for d in (1, 2, -1, -2))) + slope(
            *(at(15, dy=d) for d in (1, 2, -1, -2))
        )
        div = div + slope(
            *neighbours(GZ[op, 8 * t : 8 * t + 8, :], edge(pz[14], k))
        )
        ricci = (2.0 / 3.0) * (div - box_metric)
        ricci = ricci + (gd[0] * trace_grad[0] + gd[1] * trace_grad[1] + gd[2] * trace_grad[2])
        ricci = ricci + 2.0 * quad_c + quad_z

        chi_c = at(0)
        inv_chi = 1.0 / chi_c
        laplace = (4.0 / 3.0) * box_chi - (gd[0] * dchi[0] + gd[1] * dchi[1] + gd[2] * dchi[2])
        grad_sq = (
            u[0] * dchi[0] * dchi[0] + u[3] * dchi[1] * dchi[1] + u[5] * dchi[2] * dchi[2]
        ) + 2.0 * (
            u[1] * dchi[0] * dchi[1] + u[2] * dchi[0] * dchi[2] + u[4] * dchi[1] * dchi[2]
        )
        A = [at(7 + c) for c in range(6)]
        mixed = [
            [
                A[PAIR[i][0]] * U[0][j] + A[PAIR[i][1]] * U[1][j] + A[PAIR[i][2]] * U[2][j]
                for j in range(3)
            ]
            for i in range(3)
        ]
        K = at(13)
        ham = chi_c * ricci + 2.0 * laplace - 2.5 * grad_sq * inv_chi
        ham = ham + (2.0 / 3.0) * K * K - pair_trace(mixed, mixed, True)
        O[0, op, 8 * t : 8 * t + 8, :] = ham

        EA = []
        for c in range(7):
            f = 7 + c
            EA.append(
                (
                    slope(*(at(f, dx=d) for d in (1, 2, -1, -2))),
                    slope(*(at(f, dy=d) for d in (1, 2, -1, -2))),
                    slope(*neighbours(at(f), edge(pz[f], k))),
                )
            )
        weighted = [1.5 * inv_chi * d for d in dchi]
        mom_sq = None
        for i in range(3):
            flat = None
            for j in range(3):
                for m in range(3):
                    term = U[j][m] * EA[PAIR[m][i]][j]
                    flat = term if flat is None else flat + term
            total = (2.0 / 3.0) * (flat - (2.0 / 3.0) * EA[6][i])
            for l in range(3):
                total = total - gd[l] * A[PAIR[l][i]]
                for j in range(3):
                    total = total - C[l][PAIR[j][i]] * mixed[l][j]
                total = total - mixed[i][l] * weighted[l]
            O[1 + i, op, 8 * t : 8 * t + 8, :] = total
            mom_sq = total * total if mom_sq is None else mom_sq + total * total
        return ham * ham, mom_sq

    if edges:
        acc = (before[0], before[1])
    else:
        acc = (jnp.zeros((8, lanes), jnp.float32),) * 2
    writes = []
    base = 0
    obase = 0
    for start, count in groups:

        def one_plane(i, acc, base=base, obase=obase, start=start):
            for t in range(tiles):
                h, m = cell(base + 2 + i, start + i, obase + i, t)
                acc = (acc[0] + h, acc[1] + m)
            return acc

        acc = lax.fori_loop(0, count, one_plane, acc)
        src = pl.ds(obase, count)
        dst = pl.ds(start, count)
        writes.append(pltpu.make_async_copy(O.at[0, src], ham_out.at[dst], osem.at[len(writes)]))
        writes[-1].start()
        writes.append(
            pltpu.make_async_copy(O.at[pl.ds(1, 3), src], mom_out.at[:, dst], osem.at[len(writes)])
        )
        writes[-1].start()
        base += count + 4
        obase += count
    if edges:
        h = jnp.sum(acc[0], axis=0, keepdims=True)
        m = jnp.sum(acc[1], axis=0, keepdims=True)
        half_lane = lanes // 2
        row = lax.broadcasted_iota(jnp.int32, (1, lanes), 1)
        row = jnp.where(row < half_lane, h + pltpu.roll(h, half_lane, 1), m + pltpu.roll(m, half_lane, 1))
        sums_out[...] = jnp.broadcast_to(row, (devices, lanes))
    else:
        sums_out[0] = acc[0]
        sums_out[1] = acc[1]
    for w in writes:
        w.wait()


def hop(value, axis, step):
    n = lax.axis_size(axis)
    return lax.ppermute(value, axis, [(i, (i + step) % n) for i in range(n)])


def on_device(chi, met, cur, tra, gam):
    planes, rows, lanes = chi.shape
    devices = lax.axis_size(AXES)
    f32 = jnp.float32
    any_spec = pl.BlockSpec(memory_space=pl.ANY)
    vmem = pl.BlockSpec(memory_space=pltpu.VMEM)

    def x_all(s):
        return jnp.concatenate([chi[None, s], met[:, s], cur[:, s], tra[None, s], gam[:1, s]], 0)

    def y_all(s):
        return jnp.concatenate([c2[None, :, s], m2[:, :, s], k2[:, :, s], t2[None, :, s], g2[1:2, :, s]], 0)

    first, last = slice(0, 2), slice(planes - 2, planes)
    yfirst, ylast = slice(0, 2), slice(rows - 2, rows)
    xfirst, xlast = x_all(first), x_all(last)
    xfirst, xlast, c2, m2, k2, t2, g2 = lax.optimization_barrier((xfirst, xlast, chi, met, cur, tra, gam))
    xlo = hop(xlast, "gx", 1)
    xhi = hop(xfirst, "gx", -1)
    packed = pl.pallas_call(
        pack_kernel,
        out_shape=jax.ShapeDtypeStruct((15, 8, lanes), f32),
        in_specs=[vmem] * 5,
        out_specs=vmem,
        name="pack_z",
    )(c2, m2, k2, t2, g2)
    if lax.axis_size("gz") == 2:
        pz = hop(packed, "gz", 1)
    else:
        up = hop(packed, "gz", 1)
        down = hop(packed, "gz", -1)
        pz = jnp.where(lax.broadcasted_iota(jnp.int32, packed.shape, 2) % 4 < 2, up, down)
    ylo = hop(y_all(ylast), "gy", 1)
    yhi = hop(y_all(yfirst), "gy", -1)
    geo_z = pz[:GEO]
    pylo = hop(geo_z, "gy", 1)
    pyhi = hop(geo_z, "gy", -1)

    def small(s):
        corner = jnp.concatenate([ylo[:GEO, s].reshape(GEO, 4, lanes), yhi[:GEO, s].reshape(GEO, 4, lanes)], 1)
        return jnp.concatenate([geo_z, corner], 0)

    sxlo = hop(small(last), "gx", 1)
    sxhi = hop(small(first), "gx", -1)

    def call(groups, edges, operands, in_specs, sums_shape, aliases, name, flops):
        buf = sum(c + 4 for _, c in groups)
        outs = sum(c for _, c in groups)
        pad_rows = rows + 16
        return pl.pallas_call(
            functools.partial(main_kernel, groups, edges, planes, rows, lanes, devices),
            out_shape=(
                jax.ShapeDtypeStruct(chi.shape, f32),
                jax.ShapeDtypeStruct(gam.shape, f32),
                jax.ShapeDtypeStruct(sums_shape, f32),
            ),
            in_specs=in_specs,
            out_specs=(any_spec, any_spec, vmem),
            scratch_shapes=[
                pltpu.VMEM((16, buf, pad_rows, lanes), f32),
                pltpu.VMEM((outs, rows, lanes), f32),
                pltpu.VMEM((GEO, buf, pad_rows, lanes), f32),
                pltpu.VMEM((GEO, buf, rows, lanes), f32),
                pltpu.VMEM((GEO, outs, rows, lanes), f32),
                pltpu.VMEM((4, outs, rows, lanes), f32),
                pltpu.SemaphoreType.DMA((32,)),
                pltpu.SemaphoreType.DMA((2 * len(groups),)),
            ],
            input_output_aliases=aliases,
            cost_estimate=pl.CostEstimate(flops=flops, bytes_accessed=4 * 20 * chi.size, transcendentals=0),
            name=name,
        )(*operands)

    local = (chi, met, cur, tra, gam, ylo, yhi, pz, pylo, pyhi)
    local_specs = [any_spec] * 5 + [vmem] * 5
    work = 2000 * chi.size
    ham, mom, before = call(
        ((2, planes - 4),), False, local, local_specs, (2, 8, lanes), {}, "interior", work
    )
    ham, mom, sums = call(
        ((0, 2), (planes - 2, 2)),
        True,
        local + (xlo, xhi, sxlo, sxhi, before, ham, mom),
        local_specs + [any_spec] * 2 + [vmem] * 3 + [any_spec] * 2,
        (devices, lanes),
        {15: 0, 16: 1},
        "boundary",
        work,
    )
    parts = jnp.sum(lax.all_to_all(sums, AXES, 0, 0, tiled=True), axis=0)
    totals = jnp.stack([jnp.sum(parts[: lanes // 2]), jnp.sum(parts[lanes // 2 :])])
    cells = chi.size * devices
    norms = jnp.sqrt(totals / jnp.array([cells, 3 * cells], dtype=f32))
    return ham, mom, norms


def solution(mesh):
    return jax.shard_map(
        on_device,
        mesh=mesh,
        in_specs=(
            P("gx", "gy", "gz"),
            P(None, "gx", "gy", "gz"),
            P(None, "gx", "gy", "gz"),
            P("gx", "gy", "gz"),
            P(None, "gx", "gy", "gz"),
        ),
        out_specs=(P("gx", "gy", "gz"), P(None, "gx", "gy", "gz"), P()),
        check_vma=False,
    )
```
